32 devices in a mesh: grp: 2 (over x), aux: 16 (over z, y, core).
Axes of the slice: x: 2, y: 2, z: 4, core: 2. Of those that a mesh axis runs over, the one named last changes fastest.
Arguments:
- three_index: bfloat16 [64, 256, 256], P('aux'), may hold values from -0.375 to 0.375
- relaxed: bfloat16 [512, 256], P('grp'), parts along dimension 0, may hold values from -0.375 to 0.375
- plus_amplitude: bfloat16 [512, 256], P('grp'), parts along dimension 0, may hold values from -0.375 to 0.375
- minus_amplitude: bfloat16 [512, 256], P('grp'), parts along dimension 0, may hold values from -0.375 to 0.375
- ground: bfloat16 [256, 256], replicated, may hold values from -0.375 to 0.375
- integral_grad: bfloat16 [3, 64, 512, 256], P(None, None, 'aux'), may hold values from -0.09375 to 0.09375
- metric_grad: bfloat16 [3, 64, 64], P(None, 'aux'), may hold values from -0.5 to 0.5
- function_atom: int32 [256], replicated, may hold values from 0 to 31, never falling along the last dimension, each value on 1 to 16 neighbouring positions
- aux_center: int32 [64], P('aux'), may hold values from 0 to 31, never falling along the last dimension, each value on 1 to 4 neighbouring positions
- block_list: int32 [512], replicated, may hold values from 0 to 255, as said below
- block_count: int32 [16], replicated, may hold values from 0 to 32, as said below
Outputs:
- gradient: float32 [3, 64], P(None, 'grp'), parts along dimension 1
The draws below stay inside these ranges and needn't reach their ends.
There are 2 independent parts, one for each index of `grp`. The reference program is written for one: setup_inputs(seed, part) draws one part's arguments, and reference() takes and returns one part's arrays. A program takes and returns all parts, laid end to end along the dimension named above; an argument that names none is the same for every part. Nothing has to cross between parts.
Inputs may be any that keep to these rules, and one draw needn't show every extreme that they name: block_count[d] is the number of live slots of owner d; the counts sum to 256, and at least one owner has 32. `block_list`: slot s of owner d is entry d * 32 + s and is live when s < block_count[d]; each tile pair i * 16 + j is held by exactly one live slot; slots that are not live hold arbitrary tile pairs.
All inputs are finite; a program needn't handle non-finite values.
Results may differ from the reference program's by a relative error of at most 0.0032.
Values may be sent and summed in bfloat16 or wider, within the bound.
No kernel may reach another device: no remote copies, remote signals or barrier semaphores. Data moves between devices by JAX's collectives and lax.ppermute only.
A program may use at most 64 MiB of HBM per device.

```python
import math
import jax
import jax.numpy as jnp
import numpy as np
from jax import lax

NBW = 256
TILE = 16
NT = 16
NTP = 256
MAXT = 32
SLOTS = 512
NAUX = 64
NATOM = 32


def owner_layout(key):
    key = jax.random.fold_in(key, 7)
    first_key, second_key, third_key, fourth_key = jax.random.split(key, 4)
    owners = SLOTS // MAXT
    slot_ids = jnp.arange(SLOTS, dtype=jnp.int32)
    slot_owner = slot_ids // MAXT
    filled = jax.random.randint(first_key, (), 0, owners)
    scores = jax.random.permutation(second_key, SLOTS).astype(jnp.int32)
    scores = jnp.where(slot_owner == filled, scores - SLOTS, scores)
    ordering = jnp.argsort(scores, stable=True)
    picked = jnp.zeros((SLOTS,), jnp.int32).at[ordering[:NTP]].set(1)
    counts = picked.reshape(owners, MAXT).sum(axis=1).astype(jnp.int32)
    live_slot = slot_ids % MAXT < counts[slot_owner]
    ranking = jnp.cumsum(live_slot.astype(jnp.int32)) - 1
    tile_order = jax.random.permutation(third_key, NTP).astype(jnp.int32)
    padding = jax.random.randint(fourth_key, (SLOTS,), 0, NTP)
    listing = jnp.where(live_slot, tile_order[jnp.clip(ranking, 0, NTP - 1)], padding).astype(jnp.int32)
    return (listing, counts)


def draw_block_list(key, part):
    return owner_layout(key)[0]


def draw_block_count(key, part):
    return owner_layout(key)[1]


def block_scale(own_key, shape, pieces, low, top_value):
    gain, own = 1.0, jax.random.fold_in(own_key, 6)
    for position, parts in pieces:
        heights = jnp.exp(jax.random.uniform(jax.random.fold_in(own, position), (parts,), jnp.float32, low / len(pieces), top_value / len(pieces)))
        gain = gain * jnp.repeat(heights, shape[position] // parts).reshape([-1 if axis == position else 1 for axis in range(len(shape))])
    return gain


def split_up(count, total, bound, slope):
    portions = [(1 << 20) // math.isqrt(grade ** slope) + 1 for grade in range(2, count + 1)]
    spare, given = total - bound - (count - 1), [1] * (count - 1)
    while spare > 0:
        free = [i for i in range(count - 1) if given[i] < bound]
        pool, budget = sum([portions[i] for i in free]), spare
        for i in free:
            extra = min(bound - given[i], max(1, budget * portions[i] // pool), spare)
            given[i] = given[i] + extra
            spare = spare - extra
    return np.array([bound] + given)


def uneven_parts(stream_key, count, total, bound, lean):
    if count == 2:
        one = jax.random.randint(stream_key, (), max(1, total - bound), min(bound, total - 1) + 1)
        return jnp.stack([one, total - one])
    tallies = jnp.asarray(split_up(count, total, bound, lean), jnp.int32)
    pairs = (count - 1) // 2
    source_of, sink = tallies[1:1 + 2 * pairs:2], tallies[2:2 + 2 * pairs:2]
    margin = jnp.minimum(source_of - 1, bound - sink)
    shifted = jax.random.randint(jax.random.fold_in(stream_key, 1), (pairs,), 0, 1 << 20) % (margin + 1)
    tallies = tallies.at[1:1 + 2 * pairs:2].set(source_of - shifted).at[2:2 + 2 * pairs:2].set(sink + shifted)
    return tallies[jax.random.permutation(jax.random.fold_in(stream_key, 2), count)]


def normal_values(rng, shape, scale, reach, pieces=(), kind=jnp.bfloat16):
    factor_of = block_scale(rng, shape, pieces, -0.22, 0.18) if pieces else 1.0
    entries = jax.random.normal(rng, shape, jnp.float32) * scale * factor_of
    return jnp.minimum(jnp.maximum(entries, -reach), reach).astype(kind)


def setup_inputs(seed: int = 0, part: int = 0) -> dict:
    key_of = jax.random.split(jax.random.key(seed), 12)
    part_splits = jax.random.split(jax.random.fold_in(key_of[11], part), 12)
    return {
        "three_index": normal_values(key_of[0], (NAUX, NBW, NBW), NBW ** -0.5, 0.375, ((0, 16),)),
        "relaxed": normal_values(part_splits[1], (NBW, NBW), NBW ** -0.5, 0.375),
        "plus_amplitude": normal_values(part_splits[2], (NBW, NBW), NBW ** -0.5, 0.375),
        "minus_amplitude": normal_values(part_splits[3], (NBW, NBW), NBW ** -0.5, 0.375),
        "ground": normal_values(key_of[4], (NBW, NBW), NBW ** -0.5, 0.375),
        "integral_grad": normal_values(key_of[5], (3, NAUX, SLOTS, TILE * TILE), (NAUX * NBW // 4) ** -0.5, 0.09375, ((2, 16),)),
        "metric_grad": normal_values(key_of[6], (3, NAUX, NAUX), (NAUX * NAUX // NATOM) ** -0.5, 0.5, ((1, 16),)),
        "function_atom": jnp.searchsorted(jnp.cumsum(uneven_parts(key_of[7], NATOM, NBW, 2 * NBW // NATOM, 1)), jnp.arange(NBW), side="right").astype(jnp.int32),
        "aux_center": jnp.searchsorted(jnp.cumsum(uneven_parts(key_of[8], NATOM, NAUX, 2 * NAUX // NATOM, 1)), jnp.arange(NAUX), side="right").astype(jnp.int32),
        "block_list": draw_block_list(jax.random.fold_in(key_of[11], 71), part),
        "block_count": draw_block_count(jax.random.fold_in(key_of[11], 71), part),
    }


def reference(three_index, relaxed, plus_amplitude, minus_amplitude, ground, integral_grad, metric_grad, function_atom, aux_center, block_list, block_count):
    highest = lax.Precision.HIGHEST
    fitted = jnp.einsum('pab,ab->p', three_index.astype(jnp.float32), relaxed.astype(jnp.float32), precision=highest)
    stacked = jnp.concatenate([plus_amplitude, minus_amplitude, ground], 0)
    relaxed_wide = relaxed.astype(jnp.float32)

    def density_tiles(operands):
        slab, weight = operands
        halves = jnp.dot(stacked, slab, preferred_element_type=jnp.float32).astype(jnp.bfloat16)
        plus_half = halves[:NBW]
        minus_half = halves[NBW:2 * NBW]
        ground_half = halves[2 * NBW:]
        exchange_part = jnp.dot(plus_half, plus_amplitude.T, preferred_element_type=jnp.float32) - jnp.dot(minus_half, minus_amplitude.T, preferred_element_type=jnp.float32)
        crossed = jnp.dot(ground_half, relaxed, preferred_element_type=jnp.float32)
        triple = (weight * relaxed_wide + exchange_part + crossed + crossed.T).astype(jnp.bfloat16)
        return triple.reshape(NT, TILE, NT, TILE).transpose(0, 2, 1, 3).reshape(NTP, TILE * TILE)

    blocked = lax.map(density_tiles, (three_index, fitted))
    chosen = jnp.take(blocked, block_list, axis=1)
    slot_ids = jnp.arange(SLOTS, dtype=jnp.int32)
    live_mask = ((slot_ids % MAXT) < block_count[slot_ids // MAXT]).astype(jnp.float32)

    def contract(component):
        return jnp.sum(chosen.astype(jnp.float32) * component.astype(jnp.float32), axis=0)

    contracted = lax.map(contract, integral_grad)
    row_sums = contracted.reshape(3, SLOTS, TILE, TILE).sum(axis=3) * live_mask[None, :, None]
    function_ids = (block_list // NT)[:, None] * TILE + jnp.arange(TILE, dtype=jnp.int32)[None, :]
    atom_table = (function_atom[function_ids][:, :, None] == jnp.arange(NATOM, dtype=jnp.int32)[None, None, :]).astype(jnp.float32)
    three_part = 2.0 * jnp.einsum('kgm,gma->ka', row_sums, atom_table, precision=highest)
    coupling = jnp.einsum('kpq,q->kp', metric_grad.astype(jnp.float32), fitted, precision=highest)
    aux_table = (aux_center[:, None] == jnp.arange(NATOM, dtype=jnp.int32)[None, :]).astype(jnp.float32)
    metric_part = jnp.einsum('kp,pa->ka', coupling * fitted[None, :], aux_table, precision=highest)
    return three_part - metric_part
```

```python
import functools

import jax
import jax.numpy as jnp
from jax import lax
from jax.experimental import pallas as pl
from jax.experimental.pallas import tpu as pltpu
from jax.sharding import PartitionSpec as P

TILE = 16
NATOM = 32
LANES = 128

f32 = jnp.float32
bf16 = jnp.bfloat16


def dot(a, b, ca=1, cb=0):
    return lax.dot_general(a, b, (((ca,), (cb,)), ((), ())), preferred_element_type=f32)


def iota(shape, dim):
    return lax.broadcasted_iota(jnp.int32, shape, dim)


def swap_blocks(quadrant):
    half = LANES // TILE
    blocks = [quadrant[u * TILE : (u + 1) * TILE] for u in range(half)]
    lane = iota((TILE, LANES), 1) // TILE
    step = half // 2
    while step:
        upper = (lane // step) % 2 == 1
        for u in range(half):
            if u & step:
                continue
            low, high = blocks[u], blocks[u + step]
            blocks[u] = jnp.where(upper, pltpu.roll(high, step * TILE, 1), low)
            blocks[u + step] = jnp.where(upper, high, pltpu.roll(low, LANES - step * TILE, 1))
        step //= 2
    return jnp.concatenate(blocks, axis=0)


def density_kernel(owners, depth, *refs):
    slabs_hbm, r_hbm, x_hbm, y_hbm, g_hbm, list_hbm, out_ref, weight_ref = refs[:8]
    slab_ref, r_ref, x_ref, y_ref, g_ref, list_ref, left_ref, fixed_ref, rows_ref, pick_ref, sem = refs[8:]
    aux_local = slabs_hbm.shape[0]
    size = r_ref.shape[0]
    tiles = size // TILE
    copies = [
        pltpu.make_async_copy(source, target, sem.at[k])
        for k, (source, target) in enumerate(
            ((list_hbm, list_ref), (x_hbm, x_ref), (y_hbm, y_ref), (g_hbm, g_ref), (r_hbm, r_ref))
        )
    ]
    copies += [pltpu.make_async_copy(slabs_hbm.at[p], slab_ref.at[p], sem.at[5 + p]) for p in range(aux_local)]
    for copy in copies:
        copy.start()
    me = lax.axis_index("aux")
    row = iota((size, size), 0)
    spread = jnp.where((row % tiles) * TILE + row // tiles == iota((size, size), 1), 1.0, 0.0).astype(bf16)
    copies[0].wait()
    tile_ids = list_ref[...]
    places = (tile_ids % tiles) * tiles + tile_ids // tiles
    total = places.shape[1]
    pick_ref[...] = jnp.where(iota((tiles * tiles, total), 0) == places, 1.0, 0.0).T.astype(bf16)
    copies[1].wait()
    left_ref[0:size, :] = dot(spread, x_ref[...]).astype(bf16)
    copies[2].wait()
    left_ref[size : 2 * size, :] = -dot(spread, y_ref[...]).astype(bf16)
    copies[3].wait()
    left_ref[2 * size : 3 * size, :] = dot(spread, g_ref[...]).astype(bf16)
    left_ref[3 * size :, :] = g_ref[...]
    copies[4].wait()
    fixed_ref[...] = dot(spread, r_ref[...], 1, 1).astype(bf16)
    rows_ref[...] = dot(spread, r_ref[...])
    width = weight_ref.shape[1]
    lanes = iota((8, width), 1)
    weights_row = jnp.zeros((8, width), f32)
    for p in range(aux_local):
        copies[5 + p].wait()
        slab = slab_ref[p]
        product = slab.astype(f32) * r_ref[...].astype(f32)
        weight = jnp.sum(jnp.sum(product, axis=0, keepdims=True), axis=1, keepdims=True)
        weights_row = jnp.where(lanes == me * aux_local + p, weight, weights_row)
        halves = dot(left_ref[...], slab).astype(bf16)
        wide = jnp.concatenate([halves[0:size], halves[size : 2 * size], fixed_ref[...]], axis=1)
        right = jnp.concatenate([x_ref[...], y_ref[...], halves[3 * size :]], axis=1)
        triple = dot(wide, right, 1, 1) + dot(halves[2 * size : 3 * size], r_ref[...]) + weight * rows_ref[...]
        parts = []
        for h in range(2):
            parts.append(
                jnp.concatenate(
                    [
                        swap_blocks(triple[v * LANES : (v + 1) * LANES, h * LANES : (h + 1) * LANES])
                        for v in range(2)
                    ],
                    axis=1,
                )
            )
        blocked = jnp.concatenate(parts, axis=0).astype(bf16)
        chosen = dot(pick_ref[...], blocked).astype(bf16)
        for d in range(owners):
            out_ref[d, p * depth : (p + 1) * depth, :] = chosen[d * depth : (d + 1) * depth]
    weight_ref[...] = weights_row


def prepare_kernel(depth, *refs):
    grad_hbm, metric_hbm, atoms_hbm, centers_hbm, list_hbm, count_hbm, weight_ref = refs[:7]
    components = grad_hbm.shape[0]
    grad_refs = refs[7 : 7 + components]
    at_ref, message_ref = refs[7 + components : 9 + components]
    metric_ref, atoms_ref, centers_ref, list_ref, count_ref, table_ref, sem = refs[9 + components :]
    copies = [
        pltpu.make_async_copy(source, target, sem.at[k])
        for k, (source, target) in enumerate(
            (
                (atoms_hbm, atoms_ref),
                (list_hbm, list_ref),
                (count_hbm, count_ref),
                (metric_hbm, metric_ref),
                (centers_hbm, centers_ref),
                *((grad_hbm.at[c], grad_refs[c]) for c in range(components)),
            )
        )
    ]
    for copy in copies:
        copy.start()
    _, aux_local, aux_total = metric_ref.shape
    size = at_ref.shape[1]
    tiles = size // TILE
    me = lax.axis_index("aux")
    wide = iota((size, size), 1)
    deep = iota((size, size), 0)
    expand = jnp.where(deep % TILE == wide // TILE, 1.0, 0.0).astype(bf16)
    mine = iota((tiles, size), 1) // TILE == iota((tiles, size), 0)
    copies[0].wait()
    atoms = jnp.where(mine, jnp.broadcast_to(atoms_ref[...], (tiles, size)).astype(f32), 0.0).astype(bf16)
    table_ref[...] = dot(atoms, expand).astype(jnp.int32)
    copies[1].wait()
    copies[2].wait()
    count = count_ref[me]
    for g in range(depth):
        i = list_ref[me * depth + g] // tiles
        at_ref[g : g + 1, :] = jnp.where(g < count, table_ref[pl.ds(i, 1), :], -1)
    copies[3].wait()
    copies[4].wait()
    message_ref[...] = jnp.zeros(message_ref.shape, f32)
    weights = weight_ref[0:1, :]
    lanes = iota(weights.shape, 1)
    lane = iota((1, LANES), 1)
    for p in range(aux_local):
        weight = jnp.sum(jnp.where(lanes == me * aux_local + p, weights, 0.0), axis=1, keepdims=True)
        center = jnp.where(lane == 0, centers_ref[p].astype(f32), 0.0)
        for c in range(components):
            k = c * aux_local + p
            message_ref[k : k + 1, 0:aux_total] = weight * metric_ref[c, p : p + 1, :].astype(f32)
            message_ref[k : k + 1, aux_total : aux_total + 1] = center[:, 0:1]
    k = components * (aux_local + 1)
    message_ref[k : k + 1, :] = weights
    for copy in copies[5:]:
        copy.wait()


def gradient_kernel(depth, arrived, *refs):
    grad_refs, (at_ref, message_ref, out_ref) = refs[:-3], refs[-3:]
    components, size = len(grad_refs), arrived.shape[2]
    owners, rows, _ = arrived.shape
    aux_local = rows // depth
    sums = [jnp.zeros((depth, size), f32) for _ in range(components)]
    for d in range(owners):
        for p in range(aux_local):
            tile = arrived[d, p * depth : (p + 1) * depth, :].astype(f32)
            for c in range(components):
                sums[c] = sums[c] + tile * grad_refs[c][d * aux_local + p].astype(f32)
    at = at_ref[...]
    lane_atom = iota((1, message_ref.shape[1]), 1)
    lines = []
    for c in range(components):
        line = jnp.zeros(lane_atom.shape, f32)
        for a in range(NATOM):
            picked = jnp.sum(jnp.where(at == a, sums[c], 0.0), axis=0, keepdims=True)
            value = jnp.sum(picked, axis=1, keepdims=True)
            line = jnp.where(lane_atom == a, 2.0 * value, line)
        lines.append(line)
    base = components * aux_local
    message = message_ref[...]
    row = iota(message.shape, 0)
    for c in range(components):
        message = jnp.where(row == base + c, lines[c], message)
    for d in range(owners):
        out_ref[d] = message


def finish_kernel(components, aux_local, aux_total, arrived, out_ref):
    base = components * aux_local
    total = jnp.sum(arrived[...], axis=0)
    fitted = total[base + components : base + components + 1]
    terms = arrived[:, 0:base, :]
    coupling = jnp.sum(terms * fitted[None], axis=2, keepdims=True)
    center = terms[:, :, aux_total : aux_total + 1].astype(jnp.int32)
    lane = iota((1, 1, NATOM), 2)
    spread = jnp.sum(jnp.where(center == lane, coupling, 0.0), axis=0)
    for c in range(components):
        metric_part = jnp.sum(spread[c * aux_local : (c + 1) * aux_local], axis=0, keepdims=True)
        out_ref[c : c + 1, :] = total[base + c : base + c + 1, 0:NATOM] - metric_part


def on_device(
    owners,
    three_index,
    relaxed,
    plus_amplitude,
    minus_amplitude,
    ground,
    integral_grad,
    metric_grad,
    function_atom,
    aux_center,
    block_list,
    block_count,
):
    aux_local, size, _ = three_index.shape
    components, aux_total, depth, _ = integral_grad.shape
    tiles = size // TILE
    slots = block_list.shape[0]
    width = (aux_total // LANES + 1) * LANES
    lines = (components * (aux_local + 1) + 8) // 8 * 8
    vmem = pl.BlockSpec(memory_space=pltpu.VMEM)
    hbm = pl.BlockSpec(memory_space=pltpu.HBM)
    payload, weights = pl.pallas_call(
        functools.partial(density_kernel, owners, depth),
        out_shape=[
            jax.ShapeDtypeStruct((owners, aux_local * depth, size), bf16),
            jax.ShapeDtypeStruct((8, width), f32),
        ],
        in_specs=[hbm] * 6,
        out_specs=[vmem] * 2,
        scratch_shapes=[
            pltpu.VMEM((aux_local, size, size), bf16),
            pltpu.VMEM((size, size), bf16),
            pltpu.VMEM((size, size), bf16),
            pltpu.VMEM((size, size), bf16),
            pltpu.VMEM((size, size), bf16),
            pltpu.VMEM((1, slots), jnp.int32),
            pltpu.VMEM((4 * size, size), bf16),
            pltpu.VMEM((size, size), bf16),
            pltpu.VMEM((size, size), f32),
            pltpu.VMEM((slots, tiles * tiles), bf16),
            pltpu.SemaphoreType.DMA((5 + aux_local,)),
        ],
        compiler_params=pltpu.CompilerParams(vmem_limit_bytes=63 << 20),
        cost_estimate=pl.CostEstimate(flops=1 << 30, bytes_accessed=1 << 21, transcendentals=0),
        name="density",
    )(three_index, relaxed, plus_amplitude, minus_amplitude, ground, block_list[None, :])
    arrived = lax.all_to_all(payload, "aux", 0, 0, tiled=True)
    *grads, at, message = pl.pallas_call(
        functools.partial(prepare_kernel, depth),
        out_shape=[
            *[jax.ShapeDtypeStruct(integral_grad.shape[1:], bf16)] * components,
            jax.ShapeDtypeStruct((depth, size), jnp.int32),
            jax.ShapeDtypeStruct((lines, width), f32),
        ],
        in_specs=[hbm] * 6 + [vmem],
        out_specs=[vmem] * (2 + components),
        scratch_shapes=[
            pltpu.VMEM(metric_grad.shape, bf16),
            pltpu.VMEM((1, size), jnp.int32),
            pltpu.SMEM(aux_center.shape, jnp.int32),
            pltpu.SMEM(block_list.shape, jnp.int32),
            pltpu.SMEM(block_count.shape, jnp.int32),
            pltpu.VMEM((tiles, size), jnp.int32),
            pltpu.SemaphoreType.DMA((5 + components,)),
        ],
        compiler_params=pltpu.CompilerParams(vmem_limit_bytes=12 << 20),
        cost_estimate=pl.CostEstimate(flops=1 << 30, bytes_accessed=1 << 22, transcendentals=0),
        name="prepare",
    )(integral_grad, metric_grad, function_atom[None, :], aux_center, block_list, block_count, weights)
    partial = pl.pallas_call(
        functools.partial(gradient_kernel, depth),
        out_shape=jax.ShapeDtypeStruct((owners, lines, width), f32),
        in_specs=[vmem] * (3 + components),
        out_specs=vmem,
        compiler_params=pltpu.CompilerParams(vmem_limit_bytes=16 << 20),
        name="gradient",
    )(arrived, *grads, at, message)
    partial = lax.all_to_all(partial, "aux", 0, 0, tiled=True)
    return pl.pallas_call(
        functools.partial(finish_kernel, components, aux_local, aux_total),
        out_shape=jax.ShapeDtypeStruct((components, NATOM), f32),
        in_specs=[vmem],
        out_specs=vmem,
        name="finish",
    )(partial)


def solution(mesh):
    in_specs = (
        P("aux", None, None),
        P("grp", None),
        P("grp", None),
        P("grp", None),
        P(),
        P(None, None, "aux", None),
        P(None, "aux", None),
        P(),
        P("aux"),
        P(),
        P(),
    )
    out_specs = P(None, "grp")
    return jax.shard_map(
        functools.partial(on_device, mesh.shape["aux"]),
        mesh=mesh,
        in_specs=in_specs,
        out_specs=out_specs,
        check_vma=False,
    )
```

```python
import functools

import jax
import jax.numpy as jnp
from jax import lax
from jax.experimental import pallas as pl
from jax.experimental.pallas import tpu as pltpu
from jax.sharding import PartitionSpec as P

TILE = 16
NATOM = 32
LANES = 128


f32 = jnp.float32
bf16 = jnp.bfloat16


def shifts(chips):
    return [0, *range(chips - 1, 0, -1)]


def dot(a, b, ca=1, cb=0):
    return lax.dot_general(a, b, (((ca,), (cb,)), ((), ())), preferred_element_type=f32)


def iota(shape, dim):
    return lax.broadcasted_iota(jnp.int32, shape, dim)


def swap_blocks(quadrant):
    half = LANES // TILE
    blocks = [quadrant[u * TILE : (u + 1) * TILE] for u in range(half)]
    lane = iota((TILE, LANES), 1) // TILE
    step = half // 2
    while step:
        upper = (lane // step) % 2 == 1
        for u in range(half):
            if u & step:
                continue
            low, high = blocks[u], blocks[u + step]
            blocks[u] = jnp.where(upper, pltpu.roll(high, step * TILE, 1), low)
            blocks[u + step] = jnp.where(upper, high, pltpu.roll(low, LANES - step * TILE, 1))
        step //= 2
    return jnp.concatenate(blocks, axis=0)


def setup_kernel(chips, depth, *refs):
    slabs_hbm, r_hbm, x_hbm, y_hbm, g_hbm, list_hbm = refs[:6]
    slab_ref, r_ref, x_ref, y_ref, left_ref, fixed_ref, rows_ref, pick_ref = refs[6:14]
    list_ref, turned_ref, sem = refs[14:]
    size = r_ref.shape[0]
    tiles = size // TILE
    g_ref = left_ref.at[3 * size : 4 * size]
    copies = [
        pltpu.make_async_copy(source, target, sem.at[k])
        for k, (source, target) in enumerate(
            (
                (list_hbm, list_ref),
                (x_hbm, x_ref),
                (y_hbm, y_ref),
                (g_hbm, g_ref),
                (r_hbm, r_ref),
                (slabs_hbm, slab_ref),
            )
        )
    ]
    for copy in copies:
        copy.start()
    me = lax.axis_index("aux")
    chip, core = me // 2, me % 2
    row = iota((size, size), 0)
    spread = jnp.where((row % tiles) * TILE + row // tiles == iota((size, size), 1), 1.0, 0.0).astype(bf16)
    copies[0].wait()
    tile_ids = list_ref[...]
    places = (tile_ids % tiles) * tiles + tile_ids // tiles
    total = places.shape[1]
    turned_ref[...] = jnp.where(iota((tiles * tiles, total), 0) == places, 1.0, 0.0).T
    for n, s in enumerate(shifts(chips)):
        first = pl.multiple_of(((chip ^ s) * 2 + core) * depth, depth)
        pick_ref[n * depth : (n + 1) * depth, :] = turned_ref[pl.ds(first, depth), :].astype(bf16)
    copies[1].wait()
    left_ref[0:size, :] = dot(spread, x_ref[...]).astype(bf16)
    copies[2].wait()
    left_ref[size : 2 * size, :] = -dot(spread, y_ref[...]).astype(bf16)
    copies[3].wait()
    left_ref[2 * size : 3 * size, :] = dot(spread, g_ref[...]).astype(bf16)
    copies[4].wait()
    fixed_ref[...] = dot(spread, r_ref[...], 1, 1).astype(bf16)
    rows_ref[...] = dot(spread, r_ref[...])
    copies[5].wait()


def density_kernel(chips, depth, *refs):
    own_ref, partner_ref, r_ref, x_ref, y_ref, left_ref, fixed_ref, rows_ref, pick_ref = refs[:9]
    outs, weight_ref = refs[9:-1], refs[-1]
    aux_local = own_ref.shape[0]
    size = r_ref.shape[0]
    me = lax.axis_index("aux")
    lanes = iota(weight_ref.shape, 1)
    weights_row = jnp.zeros(weight_ref.shape, f32)
    for k in range(2 * aux_local):
        slab = own_ref[k] if k < aux_local else partner_ref[k - aux_local]
        product = slab.astype(f32) * r_ref[...].astype(f32)
        weight = jnp.sum(jnp.sum(product, axis=0, keepdims=True), axis=1, keepdims=True)
        if k < aux_local:
            weights_row = jnp.where(lanes == me * aux_local + k, weight, weights_row)
        halves = dot(left_ref[...], slab).astype(bf16)
        wide = jnp.concatenate([halves[0:size], halves[size : 2 * size], fixed_ref[...]], axis=1)
        right = jnp.concatenate([x_ref[...], y_ref[...], halves[3 * size :]], axis=1)
        triple = dot(wide, right, 1, 1) + dot(halves[2 * size : 3 * size], r_ref[...]) + weight * rows_ref[...]
        parts = []
        for h in range(2):
            parts.append(
                jnp.concatenate(
                    [
                        swap_blocks(triple[v * LANES : (v + 1) * LANES, h * LANES : (h + 1) * LANES])
                        for v in range(2)
                    ],
                    axis=1,
                )
            )
        blocked = jnp.concatenate(parts, axis=0).astype(bf16)
        chosen = dot(pick_ref[...], blocked).astype(bf16)
        for s in range(chips):
            outs[s][k * depth : (k + 1) * depth, :] = chosen[s * depth : (s + 1) * depth]
    weight_ref[...] = weights_row


def prepare_kernel(depth, *refs):
    grad_hbm, metric_hbm, atoms_hbm, centers_hbm, list_hbm, count_hbm, weight_ref = refs[:7]
    grad_ref, at_ref, message_ref = refs[7:10]
    metric_ref, atoms_ref, centers_ref, list_ref, count_ref, table_ref, sem = refs[10:]
    copies = [
        pltpu.make_async_copy(source, target, sem.at[k])
        for k, (source, target) in enumerate(
            (
                (atoms_hbm, atoms_ref),
                (list_hbm, list_ref),
                (count_hbm, count_ref),
                (metric_hbm, metric_ref),
                (centers_hbm, centers_ref),
                (grad_hbm, grad_ref),
            )
        )
    ]
    for copy in copies:
        copy.start()
    components, aux_local, aux_total = metric_ref.shape
    size = at_ref.shape[1]
    tiles = size // TILE
    me = lax.axis_index("aux")
    wide = iota((size, size), 1)
    deep = iota((size, size), 0)
    expand = jnp.where(deep % TILE == wide // TILE, 1.0, 0.0).astype(bf16)
    mine = iota((tiles, size), 1) // TILE == iota((tiles, size), 0)
    copies[0].wait()
    atoms = jnp.where(mine, jnp.broadcast_to(atoms_ref[...], (tiles, size)).astype(f32), 0.0).astype(bf16)
    table_ref[...] = dot(atoms, expand).astype(jnp.int32)
    copies[1].wait()
    copies[2].wait()
    count = count_ref[me]
    for g in range(depth):
        i = list_ref[me * depth + g] // tiles
        at_ref[g : g + 1, :] = jnp.where(g < count, table_ref[pl.ds(i, 1), :], -1)
    copies[3].wait()
    copies[4].wait()
    message_ref[...] = jnp.zeros(message_ref.shape, f32)
    weights = weight_ref[0:1, :]
    lanes = iota(weights.shape, 1)
    lane = iota((1, LANES), 1)
    for p in range(aux_local):
        weight = jnp.sum(jnp.where(lanes == me * aux_local + p, weights, 0.0), axis=1, keepdims=True)
        center = jnp.where(lane == 0, centers_ref[p].astype(f32), 0.0)
        for c in range(components):
            k = c * aux_local + p
            message_ref[k : k + 1, 0:aux_total] = weight * metric_ref[c, p : p + 1, :].astype(f32)
            message_ref[k : k + 1, aux_total : aux_total + 1] = center[:, 0:1]
    k = components * (aux_local + 1)
    message_ref[k : k + 1, :] = weights
    copies[5].wait()


def gradient_kernel(aux_local, depth, *refs):
    arrived, (grad_ref, at_ref, message_ref, out_ref) = refs[:-4], refs[-4:]
    components, size = grad_ref.shape[0], grad_ref.shape[3]
    owners = out_ref.shape[0]
    me = lax.axis_index("aux")
    chip, core = me // 2, me % 2
    sums = [jnp.zeros((depth, size), f32) for _ in range(components)]
    for s, tiles_ref in zip(shifts(len(arrived)), arrived, strict=True):
        for k in range(2 * aux_local):
            sender = (chip ^ s) * 2 + (core if k < aux_local else 1 - core)
            tile = tiles_ref[k * depth : (k + 1) * depth, :].astype(f32)
            for c in range(components):
                sums[c] = sums[c] + tile * grad_ref[c, sender * aux_local + k % aux_local].astype(f32)
    at = at_ref[...]
    lane_atom = iota((1, message_ref.shape[1]), 1)
    lines = []
    for c in range(components):
        line = jnp.zeros(lane_atom.shape, f32)
        for a in range(NATOM):
            picked = jnp.sum(jnp.where(at == a, sums[c], 0.0), axis=0, keepdims=True)
            value = jnp.sum(picked, axis=1, keepdims=True)
            line = jnp.where(lane_atom == a, 2.0 * value, line)
        lines.append(line)
    base = components * aux_local
    message = message_ref[...]
    row = iota(message.shape, 0)
    for c in range(components):
        message = jnp.where(row == base + c, lines[c], message)
    for d in range(owners):
        out_ref[d] = message


def finish_kernel(components, aux_local, aux_total, arrived, out_ref):
    base = components * aux_local
    total = jnp.sum(arrived[...], axis=0)
    fitted = total[base + components : base + components + 1]
    terms = arrived[:, 0:base, :]
    coupling = jnp.sum(terms * fitted[None], axis=2, keepdims=True)
    center = terms[:, :, aux_total : aux_total + 1].astype(jnp.int32)
    lane = iota((1, 1, NATOM), 2)
    spread = jnp.sum(jnp.where(center == lane, coupling, 0.0), axis=0)
    for c in range(components):
        metric_part = jnp.sum(spread[c * aux_local : (c + 1) * aux_local], axis=0, keepdims=True)
        out_ref[c : c + 1, :] = total[base + c : base + c + 1, 0:NATOM] - metric_part


def on_device(
    owners,
    three_index,
    relaxed,
    plus_amplitude,
    minus_amplitude,
    ground,
    integral_grad,
    metric_grad,
    function_atom,
    aux_center,
    block_list,
    block_count,
):
    aux_local, size, _ = three_index.shape
    components, aux_total, depth, _ = integral_grad.shape
    tiles = size // TILE
    slots = block_list.shape[0]
    chips = owners // 2
    width = (aux_total // LANES + 1) * LANES
    lines = (components * (aux_local + 1) + 8) // 8 * 8
    vmem = pl.BlockSpec(memory_space=pltpu.VMEM)
    hbm = pl.BlockSpec(memory_space=pltpu.HBM)
    outside = functools.partial(pltpu.with_memory_space_constraint, memory_space=pltpu.HBM)
    partner = lax.ppermute(three_index, "aux", [(i, i ^ 1) for i in range(owners)])
    own, *fixed = pl.pallas_call(
        functools.partial(setup_kernel, chips, depth),
        out_shape=[
            pltpu.VMEM((aux_local, size, size), bf16),
            pltpu.VMEM((size, size), bf16),
            pltpu.VMEM((size, size), bf16),
            pltpu.VMEM((size, size), bf16),
            pltpu.VMEM((4 * size, size), bf16),
            pltpu.VMEM((size, size), bf16),
            pltpu.VMEM((size, size), f32),
            pltpu.VMEM((chips * depth, tiles * tiles), bf16),
        ],
        in_specs=[hbm] * 6,
        out_specs=[vmem] * 8,
        scratch_shapes=[
            pltpu.VMEM((1, slots), jnp.int32),
            pltpu.VMEM((slots, tiles * tiles), f32),
            pltpu.SemaphoreType.DMA((6,)),
        ],
        compiler_params=pltpu.CompilerParams(vmem_limit_bytes=16 << 20),
        cost_estimate=pl.CostEstimate(flops=1 << 30, bytes_accessed=1 << 20, transcendentals=0),
        name="setup",
    )(*map(outside, (three_index, relaxed, plus_amplitude, minus_amplitude, ground, block_list[None, :])))
    *sent, weights = pl.pallas_call(
        functools.partial(density_kernel, chips, depth),
        out_shape=[pltpu.VMEM((2 * aux_local * depth, size), bf16)] * chips + [pltpu.VMEM((8, width), f32)],
        in_specs=[vmem] * 9,
        out_specs=[vmem] * (chips + 1),
        compiler_params=pltpu.CompilerParams(vmem_limit_bytes=24 << 20),
        cost_estimate=pl.CostEstimate(flops=1 << 31, bytes_accessed=1 << 21, transcendentals=0),
        name="density",
    )(own, partner, *fixed)
    arrived = [sent[0]]
    for n, s in enumerate(shifts(chips)[1:], 1):
        arrived.append(lax.ppermute(sent[n], "aux", [(i, i ^ (2 * s)) for i in range(owners)]))
    grads, at, message = pl.pallas_call(
        functools.partial(prepare_kernel, depth),
        out_shape=[
            pltpu.VMEM(integral_grad.shape, bf16),
            pltpu.VMEM((depth, size), jnp.int32),
            pltpu.VMEM((lines, width), f32),
        ],
        in_specs=[hbm] * 6 + [vmem],
        out_specs=[vmem] * 3,
        scratch_shapes=[
            pltpu.VMEM(metric_grad.shape, bf16),
            pltpu.VMEM((1, size), jnp.int32),
            pltpu.SMEM(aux_center.shape, jnp.int32),
            pltpu.SMEM(block_list.shape, jnp.int32),
            pltpu.SMEM(block_count.shape, jnp.int32),
            pltpu.VMEM((tiles, size), jnp.int32),
            pltpu.SemaphoreType.DMA((6,)),
        ],
        compiler_params=pltpu.CompilerParams(vmem_limit_bytes=16 << 20),
        cost_estimate=pl.CostEstimate(flops=1 << 30, bytes_accessed=1 << 22, transcendentals=0),
        name="prepare",
    )(*map(outside, (integral_grad, metric_grad, function_atom[None, :], aux_center, block_list, block_count)), weights)
    partial = pl.pallas_call(
        functools.partial(gradient_kernel, aux_local, depth),
        out_shape=jax.ShapeDtypeStruct((owners, lines, width), f32),
        in_specs=[vmem] * (chips + 3),
        out_specs=vmem,
        compiler_params=pltpu.CompilerParams(vmem_limit_bytes=16 << 20),
        name="gradient",
    )(*arrived, grads, at, message)
    partial = lax.all_to_all(partial, "aux", 0, 0, tiled=True)
    return pl.pallas_call(
        functools.partial(finish_kernel, components, aux_local, aux_total),
        out_shape=jax.ShapeDtypeStruct((components, NATOM), f32),
        in_specs=[vmem],
        out_specs=vmem,
        name="finish",
    )(partial)


def solution(mesh):
    in_specs = (
        P("aux", None, None),
        P("grp", None),
        P("grp", None),
        P("grp", None),
        P(),
        P(None, None, "aux", None),
        P(None, "aux", None),
        P(),
        P("aux"),
        P(),
        P(),
    )
    out_specs = P(None, "grp")
    return jax.shard_map(
        functools.partial(on_device, mesh.shape["aux"]),
        mesh=mesh,
        in_specs=in_specs,
        out_specs=out_specs,
        check_vma=False,
    )
```
